256 devices in a mesh: tm: 2 (over y_lo), row: 16 (over y_hi, z), col: 8 (over x, core).
Axes of the slice: x: 4, y: 4 (y_hi: 2, y_lo: 2; y = y_hi * 2 + y_lo), z: 8, core: 2. Of those that a mesh axis runs over, the one named last changes fastest.
Arguments:
- returns: bfloat16 [272, 16384], P('tm', ('row', 'col')), may hold values from -60 to 60
- window: int32 [1], replicated, may hold values from 200 to 256
- out_days: int32 [4], replicated, may hold values from 255 to 271
Outputs:
- correlation: bfloat16 [4, 16384, 16384], P(None, 'row', ('col', 'tm'))
The draws below stay inside these ranges and needn't reach their ends.
Inputs may be any that keep to these rules, and one draw needn't show every extreme that they name: One window length for all days. `out_days`: days may repeat.
All inputs are finite; a program needn't handle non-finite values.
Results may differ from the reference program's by a relative error of at most 0.001.
Values may be sent and summed in bfloat16 or wider, within the bound.
A program may use at most 128 MiB of HBM per device.

```python
import jax
import jax.numpy as jnp
from jax import lax

ASSETS = 16384
DAYS = 272
NOUT = 4


def draw_returns(key, part):
    keys = jax.random.split(jax.random.fold_in(key, 17), 5)
    day_scale = jnp.exp(jax.random.uniform(keys[0], (DAYS, 1), jnp.float32, jnp.log(0.3), jnp.log(3.0)))
    asset_scale = jnp.exp(jax.random.uniform(keys[1], (1, ASSETS), jnp.float32, jnp.log(0.5), jnp.log(5.0)))
    loading = jax.random.uniform(keys[2], (1, ASSETS), jnp.float32, 0.4, 1.6)
    market = jax.random.normal(keys[3], (DAYS, 1), jnp.float32)
    noise = jax.random.normal(keys[4], (DAYS, ASSETS), jnp.float32)
    signal = loading * market + noise
    values = jnp.clip(day_scale * asset_scale * signal, -60.0, 60.0)
    return values.astype(jnp.bfloat16)


def plant(entries, key, smallest, top_value):
    extent = entries.shape
    place = [jax.random.randint(jax.random.fold_in(key, axis), (), 0, extent[axis]) for axis in range(len(extent))]
    entries = entries.at[tuple(place)].set(smallest)
    longest = extent.index(max(extent))
    place[longest] = (place[longest] + 1) % extent[longest]
    return entries.at[tuple(place)].set(top_value)


def setup_inputs(seed: int = 0) -> dict:
    streams_of = jax.random.split(jax.random.key(seed), 4)
    return {
        "returns": draw_returns(jax.random.fold_in(streams_of[3], 71), 0),
        "window": jax.random.randint(streams_of[1], (1,), 200, 257).astype(jnp.int32),
        "out_days": plant(jax.random.randint(streams_of[2], (NOUT,), 255, DAYS), jax.random.fold_in(streams_of[2], 1), 255, DAYS - 1).astype(jnp.int32),
    }


def reference(returns, window, out_days):
    width = window[0]
    wide = width.astype(jnp.float32)
    day_ids = jnp.arange(DAYS, dtype=jnp.int32)
    inside = (day_ids[None, :] <= out_days[:, None]) & (day_ids[None, :] > out_days[:, None] - width)
    mask = jnp.where(inside, 1.0, 0.0).astype(jnp.float32)
    series = returns.astype(jnp.float32)
    first = jnp.dot(mask, series, precision=lax.Precision.HIGHEST)
    second = jnp.dot(mask, series * series, precision=lax.Precision.HIGHEST)
    scale = lax.rsqrt((second - first * first / wide) / wide + 1e-06)
    blocks = ASSETS // 512

    def one_block(index):
        start = (index * 512).astype(jnp.int32)
        rows = lax.dynamic_slice_in_dim(series, start, 512, 1)
        weighted = mask[:, :, None] * rows[None, :, :]
        gram = jnp.einsum('kda,db->kab', weighted, series, precision=lax.Precision.HIGHEST)
        first_rows = lax.dynamic_slice_in_dim(first, start, 512, 1)
        scale_rows = lax.dynamic_slice_in_dim(scale, start, 512, 1)
        cov = gram - first_rows[:, :, None] * first[:, None, :] / wide
        return (cov * scale_rows[:, :, None] * scale[:, None, :] / wide).astype(jnp.bfloat16)
    pieces = lax.map(one_block, jnp.arange(blocks, dtype=jnp.int32))
    return jnp.transpose(pieces, (1, 0, 2, 3)).reshape(NOUT, ASSETS, ASSETS)
```

```python
import jax
import jax.numpy as jnp
from jax import lax
from jax.experimental import pallas as pl
from jax.experimental.pallas import tpu as pltpu
from jax.sharding import PartitionSpec as P

MESH = pl.DeviceIdType.MESH
BF = jnp.bfloat16
F32 = jnp.float32
HALF = 136
WIDTH = 128
ROWS = 1024
ORDER = (1, 7, 2, 6, 3, 5, 4)


def place():
    row = lax.axis_index("row")
    col = lax.axis_index("col")
    return col // 2, row // 8, lax.axis_index("tm"), row % 8, col % 2


def device(x, y_hi, y_lo, z, core):
    return {"tm": y_lo, "row": y_hi * 8 + z, "col": x * 2 + core}


def gather_kernel(src, rows, cols, stage_sem, zs, zr, rs, rr, ys, yr, xs, xr):
    x, yh, yl, z, c = place()

    def slot_of(xd, y_lo, core):
        final = y_lo * 8 + x * 2 + core
        return jnp.where(xd == x, final, 16 + xd * 4 + y_lo * 2 + core)

    def matched(zz):
        return jnp.logical_and(zz % 2 == yl, (zz // 2) % 2 == c)

    def lies(zz):
        return jnp.where(matched(zz), slot_of(2 * yh + zz // 4, yl, c), 32 + zz)

    own = yl * 8 + x * 2 + c
    mine = lies(z)

    stages = []
    for n, (ref, at) in enumerate(((rows, own), (cols, mine))):
        first = pltpu.make_async_copy(
            src.at[pl.ds(pl.multiple_of(yl * 120, 8), 16)], ref.at[at, pl.ds(0, 16)], stage_sem.at[2 * n]
        )
        rest = pltpu.make_async_copy(
            src.at[pl.ds(pl.multiple_of(16 - yl * 16, 8), 120)], ref.at[at, pl.ds(16, 120)], stage_sem.at[2 * n + 1]
        )
        first.start()
        rest.start()
        stages += [first, rest]

    plane = [(dx, dl, dc) for dx in (0, 1, 3, 2) for dl in (0, 1) for dc in (0, 1)][1:]

    def in_plane(dx, dl, dc):
        return device((x + dx) % 4, yh, (yl + dl) % 2, z, (c + dc) % 2)

    barrier = pltpu.get_barrier_semaphore()
    partners = [in_plane(*d) for d in plane]
    partners += [device(x, yh, yl, (z + d) % 8, c) for d in ORDER]
    partners += [device(x, 1 - yh, (yl + dl) % 2, z, (c + dc) % 2) for dl in (0, 1) for dc in (0, 1)]
    for partner in partners:
        pl.semaphore_signal(barrier, inc=1, device_id=partner, device_id_type=MESH)
    for stage in stages:
        stage.wait()
    pl.semaphore_wait(barrier, len(partners))

    z_out, z_in = [], []
    for n, d in enumerate(ORDER):
        copy = pltpu.make_async_remote_copy(
            src_ref=rows.at[own],
            dst_ref=cols.at[mine],
            send_sem=zs.at[n],
            recv_sem=zr.at[n],
            device_id=device(x, yh, yl, (z + d) % 8, c),
            device_id_type=MESH,
        )
        copy.start()
        z_out.append(copy)
        z_in.append(
            pltpu.make_async_remote_copy(
                src_ref=rows.at[own],
                dst_ref=cols.at[lies((z + 8 - d) % 8)],
                send_sem=zs.at[n],
                recv_sem=zr.at[n],
                device_id=device(x, yh, yl, (z + d) % 8, c),
                device_id_type=MESH,
            )
        )

    r_out, r_in = [], []
    for n, d in enumerate(plane):
        dx, dl, dc = d
        r_out.append(
            pltpu.make_async_remote_copy(
                src_ref=rows.at[own],
                dst_ref=rows.at[own],
                send_sem=rs.at[n],
                recv_sem=rr.at[n],
                device_id=in_plane(*d),
                device_id_type=MESH,
            )
        )
        r_out[-1].start()
        from_x, from_l, from_c = (x + 4 - dx) % 4, (yl + dl) % 2, (c + dc) % 2
        r_in.append(
            pltpu.make_async_remote_copy(
                src_ref=rows.at[own],
                dst_ref=rows.at[from_l * 8 + from_x * 2 + from_c],
                send_sem=rs.at[n],
                recv_sem=rr.at[n],
                device_id=in_plane(*d),
                device_id_type=MESH,
            )
        )

    def y_copy(step, j, zz):
        xd = 2 * yh + zz // 4
        to_h = (yh + j) % 2
        to = slot_of(xd, yl, c)
        return pltpu.make_async_remote_copy(
            src_ref=cols.at[lies(zz)],
            dst_ref=cols.at[to],
            send_sem=ys.at[2 * step + j],
            recv_sem=yr.at[xd * 4 + yl * 2 + c],
            device_id=device(x, to_h, zz % 2, z, (zz // 2) % 2),
            device_id_type=MESH,
        )

    def y_send(step, zz):
        y_copy(step, 1, zz).start()

        @pl.when(jnp.logical_not(matched(zz)))
        def _():
            y_copy(step, 0, zz).start()

    def y_sent(step, zz):
        y_copy(step, 1, zz).wait_send()

        @pl.when(jnp.logical_not(matched(zz)))
        def _():
            y_copy(step, 0, zz).wait_send()

    low = c * 2 + yl
    near = (((z + 8 - low) % 8 + 2) // 4) % 2

    def y_wait(xd, y_lo, core):
        here = jnp.logical_and(xd // 2 == yh, jnp.logical_and(y_lo == yl, core == c))

        @pl.when(jnp.logical_not(here))
        def _():
            pltpu.make_async_remote_copy(
                src_ref=rows.at[own],
                dst_ref=cols.at[slot_of(xd, y_lo, core)],
                send_sem=ys.at[0],
                recv_sem=yr.at[xd * 4 + y_lo * 2 + core],
                device_id=device(x, 1 - yh, yl, z, c),
                device_id_type=MESH,
            ).wait_recv()

    def x_copy(xd, y_lo):
        return pltpu.make_async_remote_copy(
            src_ref=cols.at[pl.ds(16 + xd * 4 + y_lo * 2, 2)],
            dst_ref=cols.at[pl.ds(y_lo * 8 + x * 2, 2)],
            send_sem=xs.at[xd * 2 + y_lo],
            recv_sem=xr.at[x * 2 + y_lo],
            device_id=device(xd, yh, yl, z, c),
            device_id_type=MESH,
        )

    def x_send(which):
        for half in (0, 1):
            xd = half * 2 + which
            for y_lo in (0, 1):
                y_wait(xd, y_lo, 0)
                y_wait(xd, y_lo, 1)

                @pl.when(xd != x)
                def _():
                    x_copy(xd, y_lo).start()

    y_send(0, z)
    for n, d in enumerate(ORDER):
        z_in[n].wait_recv()
        y_send(n + 1, (z + 8 - d) % 8)
        if n == 4:
            x_send(near)
    x_send(1 - near)

    for copy in r_in:
        copy.wait_recv()
    for dx in (1, 3, 2):
        for y_lo in (0, 1):
            from_x = (x + dx) % 4
            pltpu.make_async_remote_copy(
                src_ref=cols.at[pl.ds(0, 2)],
                dst_ref=cols.at[pl.ds(y_lo * 8 + from_x * 2, 2)],
                send_sem=xs.at[0],
                recv_sem=xr.at[from_x * 2 + y_lo],
                device_id=device(from_x, yh, yl, z, c),
                device_id_type=MESH,
            ).wait_recv()
    for copy in z_out + r_out:
        copy.wait_send()
    for n, d in enumerate((0, *ORDER)):
        y_sent(n, (z + 8 - d) % 8)
    for dx in (1, 3, 2):
        for y_lo in (0, 1):
            x_copy((x + dx) % 4, y_lo).wait_send()


def gather(block):
    return pl.pallas_call(
        gather_kernel,
        out_shape=(pltpu.VMEM((16, HALF, WIDTH), BF), pltpu.VMEM((40, HALF, WIDTH), BF)),
        in_specs=[pl.BlockSpec(memory_space=pl.ANY)],
        out_specs=(pl.BlockSpec(memory_space=pltpu.VMEM),) * 2,
        scratch_shapes=[
            pltpu.SemaphoreType.DMA((4,)),
            pltpu.SemaphoreType.DMA((7,)),
            pltpu.SemaphoreType.DMA((7,)),
            pltpu.SemaphoreType.DMA((15,)),
            pltpu.SemaphoreType.DMA((15,)),
            pltpu.SemaphoreType.DMA((16,)),
            pltpu.SemaphoreType.DMA((16,)),
            pltpu.SemaphoreType.DMA((8,)),
            pltpu.SemaphoreType.DMA((8,)),
        ],
        compiler_params=pltpu.CompilerParams(collective_id=0, has_side_effects=True),
        name="gather",
    )(block)


def unpack(ref, flat, folded):
    for j in range(8):
        lanes = pl.ds(j * WIDTH, WIDTH)
        flat[0:128, lanes] = ref[j, 0:128]
        flat[128:240, lanes] = ref[8 + j, 16:128]
        flat[240:248, lanes] = ref[j, 128:136]
        flat[248:256, lanes] = ref[8 + j, 128:136]
        folded[0:16, lanes] = ref[8 + j, 0:16]


def day_of(spot):
    return jnp.where(
        spot < 128, spot, jnp.where(spot < 240, spot + 8, jnp.where(spot < 248, spot - 112, spot))
    )


def correlate_kernel(window, days, row_ref, col_ref, out, a, a_fold, at, at_fold, atk, b, b_fold, bk, tiles, sem):
    width = window[0]
    wide = width.astype(F32)

    def inside(day, k):
        last = days[k]
        return jnp.logical_and(day <= last, day > last - width)

    def picks(shape, axis, k, fold):
        spot = lax.broadcasted_iota(jnp.int32, shape, axis)
        if fold:
            hit = jnp.logical_and(spot < 16, inside(spot + 256, k))
        else:
            hit = inside(day_of(spot), k)
        return jnp.where(hit, 1.0, 0.0).astype(F32)

    def masks(places, fold):
        row = lax.broadcasted_iota(jnp.int32, (16, places), 0)
        total = jnp.zeros((16, places), F32)
        for k in range(4):
            total = jnp.where(row == k, picks((16, places), 1, k, fold), total)
        return total.astype(BF)

    main_mask = masks(256, False)
    fold_mask = masks(16, True)

    def sums(flat, folded):
        first = jnp.zeros((16, ROWS), F32)
        second = jnp.zeros((16, ROWS), F32)
        for ref, mask in ((flat, main_mask), (folded, fold_mask)):
            block = ref[...]
            first += jnp.dot(mask, block, preferred_element_type=F32)
            wide_block = block.astype(F32)
            square = wide_block * wide_block
            high = square.astype(BF)
            low = (square - high.astype(F32)).astype(BF)
            second += jnp.dot(mask, high, preferred_element_type=F32)
            second += jnp.dot(mask, low, preferred_element_type=F32)
        scale = lax.rsqrt((second - first * first / wide) / wide + 1e-06)
        return first, scale

    unpack(row_ref, a, a_fold)
    unpack(col_ref, b, b_fold)
    a_fold[16:128, :] = jnp.zeros((112, ROWS), BF)
    for j in range(8):
        lanes = pl.ds(j * WIDTH, WIDTH)
        at[lanes, 0:128] = jnp.transpose(a[0:128, lanes])
        at[lanes, 128:256] = jnp.transpose(a[128:256, lanes])
        at_fold[lanes, :] = jnp.transpose(a_fold[:, lanes])
    first_c, scale_c = sums(b, b_fold)
    first_c = first_c / wide
    scale_c = scale_c / wide
    first_r, scale_r = sums(a, a_fold.at[0:16])
    pad = jnp.zeros((96, ROWS), F32)
    turned = jnp.transpose(jnp.concatenate([first_r, scale_r, pad], axis=0))

    bk[16:256, :] = b[16:256, :]
    copies = []
    for k in range(4):
        pick = picks((16, 1), 0, k, False).astype(BF)
        pick_fold = picks((16, 1), 0, k, True).astype(BF)
        bk[0:16, :] = b[0:16, :] * pick + b_fold[...] * pick_fold
        main = picks((1, 256), 1, k, False).astype(BF)
        fold = picks((1, 128), 1, k, True).astype(BF)
        atk[:, 0:128] = at[:, 0:128] * main[:, 0:128] + at_fold[...] * fold
        atk[:, 128:256] = at[:, 128:256] * main[:, 128:256]
        for m in range(4):
            part = slice(m * 256, (m + 1) * 256)
            gram = jnp.dot(atk[part, :], bk[...], preferred_element_type=F32)
            mean = turned[part, k : k + 1] * first_c[k : k + 1, :]
            value = (gram - mean) * turned[part, 16 + k : 17 + k] * scale_c[k : k + 1, :]
            tiles[k, part, :] = value.astype(BF)
            copy = pltpu.make_async_copy(tiles.at[k, pl.ds(m * 256, 256)], out.at[k, pl.ds(m * 256, 256)], sem.at[k * 4 + m])
            copy.start()
            copies.append(copy)
    for copy in copies:
        copy.wait()


def correlate(window, out_days, row_pieces, col_pieces):
    return pl.pallas_call(
        correlate_kernel,
        out_shape=jax.ShapeDtypeStruct((4, ROWS, ROWS), BF),
        in_specs=[pl.BlockSpec(memory_space=pltpu.SMEM)] * 2 + [pl.BlockSpec(memory_space=pltpu.VMEM)] * 2,
        out_specs=pl.BlockSpec(memory_space=pl.ANY),
        scratch_shapes=[
            pltpu.VMEM((256, ROWS), BF),
            pltpu.VMEM((128, ROWS), BF),
            pltpu.VMEM((ROWS, 256), BF),
            pltpu.VMEM((ROWS, 128), BF),
            pltpu.VMEM((ROWS, 256), BF),
            pltpu.VMEM((256, ROWS), BF),
            pltpu.VMEM((16, ROWS), BF),
            pltpu.VMEM((256, ROWS), BF),
            pltpu.VMEM((4, ROWS, ROWS), BF),
            pltpu.SemaphoreType.DMA((16,)),
        ],
        compiler_params=pltpu.CompilerParams(vmem_limit_bytes=48 << 20),
        name="correlate",
    )(window, out_days, row_pieces, col_pieces)


def on_device(returns, window, out_days):
    row_pieces, col_pieces = gather(returns)
    return correlate(window, out_days, row_pieces, col_pieces)


def solution(mesh):
    return jax.shard_map(
        on_device,
        mesh=mesh,
        in_specs=(P("tm", ("row", "col")), P(), P()),
        out_specs=P(None, "row", ("col", "tm")),
        check_vma=False,
    )
```

```python
import jax
import jax.numpy as jnp
from jax import lax
from jax.experimental import pallas as pl
from jax.experimental.pallas import tpu as pltpu
from jax.sharding import PartitionSpec as P

MESH = pl.DeviceIdType.MESH
BF = jnp.bfloat16
F32 = jnp.float32
HALF = 136
WIDTH = 128
ROWS = 1024
NEAR = (0, 3, 1, 2)


def place():
    row = lax.axis_index("row")
    col = lax.axis_index("col")
    return col >> 1, row >> 3, lax.axis_index("tm"), row & 7, col & 1


def device(x, y_hi, y_lo, z, core):
    return {"tm": y_lo, "row": y_hi * 8 + z, "col": x * 2 + core}


def bit(value, n):
    return (value >> n) & 1


def exchange(src, buf, stage_sem, zs, zr, cs, cr, rs, rr, ds, dr, during):
    x, yh, yl, z, c = place()
    own = yl * 8 + x * 2 + c

    stages = [
        pltpu.make_async_copy(
            src.at[pl.ds(pl.multiple_of(yl * 120, 8), 16)], buf.at[own, pl.ds(0, 16)], stage_sem.at[0]
        ),
        pltpu.make_async_copy(
            src.at[pl.ds(pl.multiple_of(16 - yl * 16, 8), 120)], buf.at[own, pl.ds(16, 120)], stage_sem.at[1]
        ),
    ]
    for stage in stages:
        stage.start()

    def remote(at, to, send, recv, target):
        return pltpu.make_async_remote_copy(
            src_ref=buf.at[at],
            dst_ref=buf.at[to],
            send_sem=send,
            recv_sem=recv,
            device_id=target,
            device_id_type=MESH,
        )

    beside = 1 - 2 * c

    def relay_to(i):
        to = (z + 2 * i + c) & 7
        return device(x, (yh + bit(z, 1) + bit(to, 1)) & 1, yl, to, c)

    def relay_from(i):
        at = (z + 8 - 2 * i - c) & 7
        return at, (yh + bit(z, 1) + bit(at, 1)) & 1

    def needs(i, half, step):
        at, high = relay_from(i)
        return device(2 * high + (at >> 2), (yh + half) & 1, at & 1, (z + 8 + beside * step) & 7, bit(at, 1))

    def needed_here(i):
        at, high = relay_from(i)
        return (2 * high + (at >> 2) == x) & (at & 1 == yl) & (bit(at, 1) == c)

    wanted = 4 * (x & 1) + 2 * c + yl

    def relay_at(half, x_from, core):
        same = (z + wanted + core) & 1 == 0
        at = jnp.where(same, z, (z + 7 + 2 * core) & 7)
        return at, ((x >> 1) + bit(wanted, 1) + bit(at, 1)) & 1

    def relay_is_here(half, x_from, core):
        at, high = relay_at(half, x_from, core)
        return (at == z) & (high == yh) & (half == yl) & (x_from == x) & (core == c)

    pieces = [(half, step, core) for step in (0, 1, 3, 2) for half in (0, 1) for core in (0, 1)]

    def relay_device(half, x_from, core):
        at, high = relay_at(half, x_from, core)
        return device(x_from, high, half, at, core)

    def near_by(dx, dl, dc):
        return device((x + dx) & 3, yh, (yl + dl) & 1, z, (c + dc) & 1)

    barrier = pltpu.get_barrier_semaphore()

    def greet(target):
        pl.semaphore_signal(barrier, inc=1, device_id=target, device_id_type=MESH)

    for i in (2, 1, 3):
        at, high = relay_from(i)
        greet(device(x, high, yl, at, c))

    @pl.when(c == 1)
    def _():
        at, high = relay_from(0)
        greet(device(x, high, yl, at, c))

    for half, step, core in pieces:
        x_from = (x + step) & 3
        if step == 0:

            @pl.when(jnp.logical_not(relay_is_here(half, x_from, core)))
            def _():
                greet(relay_device(half, x_from, core))

        else:
            greet(relay_device(half, x_from, core))
    for d in ((0, 1, 0), (1, 0, 0), (3, 0, 0), (2, 0, 0), (0, 0, 1)):
        greet(near_by(*d))
    kept = sum(jnp.where(needed_here(i), 1, 0) for i in range(4))
    for stage in stages:
        stage.wait()
    pl.semaphore_wait(barrier, 3 + c + 16 - kept + 5)

    sent = []

    def send(copy, when=None):
        if when is None:
            copy.start()
        else:

            @pl.when(when)
            def _():
                copy.start()

        sent.append((copy, when))

    def relay_copy(i):
        return remote(own, 32 + i, zs.at[i], zr.at[i], relay_to(i))

    for i in NEAR:
        send(relay_copy(i), c == 1 if i == 0 else None)

    mate = (1 - yl) * 8 + x * 2 + c

    def slot(half, x_from, core):
        return half * 8 + x_from * 2 + core

    def row_copy(n, at, d):
        return remote(at, at, rs.at[n], rr.at[n], near_by(*d))

    def core_copy(n, at):
        return remote(at, at, ds.at[n], dr.at[n], near_by(0, 0, 1))

    send(row_copy(0, own, (0, 1, 0)))
    for n, dx in enumerate((1, 3, 2)):
        send(row_copy(1 + n, own, (dx, 0, 0)))
    send(core_copy(0, own))

    def forward(i):
        at = jnp.where(c == 0, own, 32) if i == 0 else 32 + i
        here = needed_here(i)
        for step in (1, 0):
            for half in (1, 0):
                copy = remote(at, 16 + own, cs.at[4 * i + 2 * half + step], cr.at[own], needs(i, half, step))
                if step or half:
                    send(copy)
                else:
                    send(copy, jnp.logical_not(here))

                    @pl.when(here)
                    def _():
                        buf[16 + own] = buf[at]

    for n, i in enumerate(NEAR):
        if i == 0:

            @pl.when(c == 1)
            def _():
                relay_copy(0).wait_recv()

        else:
            relay_copy(i).wait_recv()
        forward(i)
        if n == 0:
            row_copy(0, mate, (0, 1, 0)).wait_recv()
            for k, dx in enumerate((1, 3, 2)):
                send(row_copy(4 + k, mate, (dx, 0, 0)))
            send(core_copy(1, mate))
    for n, dx in enumerate((1, 3, 2)):
        x_from = (x + 4 - dx) & 3
        for k, half in enumerate((yl, 1 - yl)):
            at = slot(half, x_from, c)
            row_copy(1 + n + 3 * k, at, (dx, 0, 0)).wait_recv()
            send(core_copy(2 + 2 * n + k, at))
    core_copy(0, slot(yl, x, 1 - c)).wait_recv()
    core_copy(1, slot(1 - yl, x, 1 - c)).wait_recv()
    for n, dx in enumerate((1, 3, 2)):
        for k, half in enumerate((yl, 1 - yl)):
            core_copy(2 + 2 * n + k, slot(half, (x + 4 - dx) & 3, 1 - c)).wait_recv()

    during()

    for half, step, core in pieces:
        x_from = (x + step) & 3
        at = slot(half, x_from, core)
        copy = remote(own, 16 + at, cs.at[0], cr.at[at], relay_device(half, x_from, core))
        if step == 0:

            @pl.when(jnp.logical_not(relay_is_here(half, x_from, core)))
            def _():
                copy.wait_recv()

        else:
            copy.wait_recv()
    for copy, when in sent:
        if when is None:
            copy.wait_send()
        else:

            @pl.when(when)
            def _():
                copy.wait_send()


def unpack(ref, first, flat, folded):
    for j in range(8):
        lanes = pl.ds(j * WIDTH, WIDTH)
        flat[0:128, lanes] = ref[first + j, 0:128]
        flat[128:240, lanes] = ref[first + 8 + j, 16:128]
        flat[240:248, lanes] = ref[first + j, 128:136]
        flat[248:256, lanes] = ref[first + 8 + j, 128:136]
        folded[0:16, lanes] = ref[first + 8 + j, 0:16]


def picks(shape, axis, window, last, fold):
    spot = lax.broadcasted_iota(jnp.int32, shape, axis)
    if fold:
        day = jnp.where(spot < 16, spot + 256, 1 << 20)
    else:
        day = jnp.where(
            spot < 128, spot, jnp.where(spot < 240, spot + 8, jnp.where(spot < 248, spot - 112, spot))
        )
    return jnp.where((day <= last) & (day > last - window), 1.0, 0.0).astype(F32)


def sums(flat, folded, main_mask, fold_mask, wide):
    first = jnp.zeros((16, ROWS), F32)
    second = jnp.zeros((16, ROWS), F32)
    for ref, mask in ((flat, main_mask), (folded, fold_mask)):
        block = ref[...]
        first += jnp.dot(mask, block, preferred_element_type=F32)
        wide_block = block.astype(F32)
        square = wide_block * wide_block
        high = square.astype(BF)
        low = (square - high.astype(F32)).astype(BF)
        second += jnp.dot(mask, high, preferred_element_type=F32)
        second += jnp.dot(mask, low, preferred_element_type=F32)
    scale = lax.rsqrt((second - first * first / wide) / wide + 1e-06)
    return first, scale


def gather_kernel(
    src, window, days_hbm,
    buf, left, turned, masks, folds, widths,
    days, a, a_fold, at, at_fold, small_sem, *sems,
):
    get_days = pltpu.make_async_copy(days_hbm, days, small_sem.at[0])
    get_days.start()

    def during():
        get_days.wait()
        width = window[0]
        wide = width.astype(F32)
        widths[...] = jnp.full((8, WIDTH), wide, F32)
        row = lax.broadcasted_iota(jnp.int32, (16, 256), 0)
        main = jnp.zeros((16, 256), F32)
        fold = jnp.zeros((16, 256), F32)
        for k in range(4):
            main = jnp.where(row == k, picks((16, 256), 1, width, days[k], False), main)
            fold = jnp.where(row == k, picks((16, 256), 1, width, days[k], True), fold)
            folds[2 * k] = picks((16, WIDTH), 0, width, days[k], False).astype(BF)
            folds[2 * k + 1] = picks((16, WIDTH), 0, width, days[k], True).astype(BF)
        masks[0:16, :] = main.astype(BF)
        masks[16:32, :] = fold.astype(BF)

        unpack(buf, 0, a, a_fold)
        a_fold[16:128, :] = jnp.zeros((112, ROWS), BF)
        for j in range(8):
            lanes = pl.ds(j * WIDTH, WIDTH)
            at[lanes, 0:128] = jnp.transpose(a[0:128, lanes])
            at[lanes, 128:256] = jnp.transpose(a[128:256, lanes])
            at_fold[lanes, :] = jnp.transpose(a_fold[:, lanes])
        first, scale = sums(a, a_fold.at[0:16], masks[0:16, :], masks[16:32, 0:16], wide)
        pad = jnp.zeros((96, ROWS), F32)
        turned[...] = jnp.transpose(jnp.concatenate([first, scale, pad], axis=0))
        for k in range(4):
            main = picks((1, 256), 1, width, days[k], False).astype(BF)
            fold = picks((1, 128), 1, width, days[k], True).astype(BF)
            left[k, :, 0:128] = at[:, 0:128] * main[:, 0:128] + at_fold[...] * fold
            left[k, :, 128:256] = at[:, 128:256] * main[:, 128:256]

    exchange(src, buf, *sems, during)


def gather(block, window, out_days):
    vmem = pl.BlockSpec(memory_space=pltpu.VMEM)
    hbm = pl.BlockSpec(memory_space=pltpu.HBM)
    return pl.pallas_call(
        gather_kernel,
        out_shape=(
            pltpu.VMEM((36, HALF, WIDTH), BF),
            pltpu.VMEM((4, ROWS, 256), BF),
            pltpu.VMEM((ROWS, WIDTH), F32),
            pltpu.VMEM((32, 256), BF),
            pltpu.VMEM((8, 16, WIDTH), BF),
            pltpu.VMEM((8, WIDTH), F32),
        ),
        in_specs=[hbm, pl.BlockSpec(memory_space=pltpu.SMEM), hbm],
        out_specs=(vmem,) * 6,
        scratch_shapes=[
            pltpu.SMEM((4,), jnp.int32),
            pltpu.VMEM((256, ROWS), BF),
            pltpu.VMEM((128, ROWS), BF),
            pltpu.VMEM((ROWS, 256), BF),
            pltpu.VMEM((ROWS, 128), BF),
            pltpu.SemaphoreType.DMA((1,)),
        ]
        + [pltpu.SemaphoreType.DMA((n,)) for n in (2, 4, 4, 16, 16, 7, 7, 8, 8)],
        compiler_params=pltpu.CompilerParams(collective_id=0, has_side_effects=True, vmem_limit_bytes=16 << 20),
        name="gather",
    )(block, window, out_days)


def correlate_kernel(buf, left, turned, masks, folds, widths, out, b, b_fold, bk, tiles, sem):
    wide = widths[0:1, 0:1]
    unpack(buf, 16, b, b_fold)
    first, scale = sums(b, b_fold, masks[0:16, :], masks[16:32, 0:16], wide)
    first = first / wide
    scale = scale / wide
    bk[16:256, :] = b[16:256, :]
    copies = []
    for k in range(4):
        for j in range(8):
            lanes = pl.ds(j * WIDTH, WIDTH)
            bk[0:16, lanes] = b[0:16, lanes] * folds[2 * k] + b_fold[:, lanes] * folds[2 * k + 1]
        for m in range(4):
            part = slice(m * 256, (m + 1) * 256)
            gram = jnp.dot(left[k, part, :], bk[...], preferred_element_type=F32)
            mean = turned[part, k : k + 1] * first[k : k + 1, :]
            value = (gram - mean) * turned[part, 16 + k : 17 + k] * scale[k : k + 1, :]
            tiles[k, part, :] = value.astype(BF)
            copy = pltpu.make_async_copy(
                tiles.at[k, pl.ds(m * 256, 256)], out.at[k, pl.ds(m * 256, 256)], sem.at[k * 4 + m]
            )
            copy.start()
            copies.append(copy)
    for copy in copies:
        copy.wait()


def correlate(*operands):
    return pl.pallas_call(
        correlate_kernel,
        out_shape=jax.ShapeDtypeStruct((4, ROWS, ROWS), BF),
        in_specs=[pl.BlockSpec(memory_space=pltpu.VMEM)] * 6,
        out_specs=pl.BlockSpec(memory_space=pl.ANY),
        scratch_shapes=[
            pltpu.VMEM((256, ROWS), BF),
            pltpu.VMEM((16, ROWS), BF),
            pltpu.VMEM((256, ROWS), BF),
            pltpu.VMEM((4, ROWS, ROWS), BF),
            pltpu.SemaphoreType.DMA((16,)),
        ],
        compiler_params=pltpu.CompilerParams(vmem_limit_bytes=32 << 20),
        name="correlate",
    )(*operands)


def on_device(returns, window, out_days):
    returns = pltpu.with_memory_space_constraint(returns, pltpu.HBM)
    out_days = pltpu.with_memory_space_constraint(out_days, pltpu.HBM)
    return correlate(*gather(returns, window, out_days))


def solution(mesh):
    return jax.shard_map(
        on_device,
        mesh=mesh,
        in_specs=(P("tm", ("row", "col")), P(), P()),
        out_specs=P(None, "row", ("col", "tm")),
        check_vma=False,
    )
```

```python
import jax
import jax.numpy as jnp
from jax import lax
from jax.experimental import pallas as pl
from jax.experimental.pallas import tpu as pltpu
from jax.sharding import PartitionSpec as P

MESH = pl.DeviceIdType.MESH
BF = jnp.bfloat16
F32 = jnp.float32
HALF = 136
WIDTH = 128
ROWS = 1024
NEAR = (0, 3, 1, 2)


def place():
    row = lax.axis_index("row")
    col = lax.axis_index("col")
    return col >> 1, row >> 3, lax.axis_index("tm"), row & 7, col & 1


def device(x, y_hi, y_lo, z, core):
    return {"tm": y_lo, "row": y_hi * 8 + z, "col": x * 2 + core}


def bit(value, n):
    return (value >> n) & 1


def exchange(src, buf, stage_sem, zs, zr, cs, cr, rs, rr, ds, dr, during):
    x, yh, yl, z, c = place()
    own = yl * 8 + x * 2 + c

    stages = [
        pltpu.make_async_copy(
            src.at[pl.ds(pl.multiple_of(yl * 120, 8), 16)], buf.at[own, pl.ds(0, 16)], stage_sem.at[0]
        ),
        pltpu.make_async_copy(
            src.at[pl.ds(pl.multiple_of(16 - yl * 16, 8), 120)], buf.at[own, pl.ds(16, 120)], stage_sem.at[1]
        ),
    ]
    for stage in stages:
        stage.start()

    def remote(at, to, send, recv, target):
        return pltpu.make_async_remote_copy(
            src_ref=buf.at[at],
            dst_ref=buf.at[to],
            send_sem=send,
            recv_sem=recv,
            device_id=target,
            device_id_type=MESH,
        )

    beside = 1 - 2 * c

    def relay_to(i):
        to = (z + 2 * i + c) & 7
        return device(x, (yh + bit(z, 1) + bit(to, 1)) & 1, yl, to, c)

    def relay_from(i):
        at = (z + 8 - 2 * i - c) & 7
        return at, (yh + bit(z, 1) + bit(at, 1)) & 1

    def needs(i, half, step):
        at, high = relay_from(i)
        return device(2 * high + (at >> 2), (yh + half) & 1, at & 1, (z + 8 + beside * step) & 7, bit(at, 1))

    def needed_here(i):
        at, high = relay_from(i)
        return (2 * high + (at >> 2) == x) & (at & 1 == yl) & (bit(at, 1) == c)

    wanted = 4 * (x & 1) + 2 * c + yl

    def relay_at(half, x_from, core):
        same = (z + wanted + core) & 1 == 0
        at = jnp.where(same, z, (z + 7 + 2 * core) & 7)
        return at, ((x >> 1) + bit(wanted, 1) + bit(at, 1)) & 1

    def relay_is_here(half, x_from, core):
        at, high = relay_at(half, x_from, core)
        return (at == z) & (high == yh) & (half == yl) & (x_from == x) & (core == c)

    pieces = [(half, step, core) for step in (0, 1, 3, 2) for half in (0, 1) for core in (0, 1)]

    def relay_device(half, x_from, core):
        at, high = relay_at(half, x_from, core)
        return device(x_from, high, half, at, core)

    def near_by(dx, dl, dc):
        return device((x + dx) & 3, yh, (yl + dl) & 1, z, (c + dc) & 1)

    barrier = pltpu.get_barrier_semaphore()

    def greet(target):
        pl.semaphore_signal(barrier, inc=1, device_id=target, device_id_type=MESH)

    for i in (2, 1, 3):
        at, high = relay_from(i)
        greet(device(x, high, yl, at, c))

    @pl.when(c == 1)
    def _():
        at, high = relay_from(0)
        greet(device(x, high, yl, at, c))

    for half, step, core in pieces:
        x_from = (x + step) & 3
        if step == 0:

            @pl.when(jnp.logical_not(relay_is_here(half, x_from, core)))
            def _():
                greet(relay_device(half, x_from, core))

        else:
            greet(relay_device(half, x_from, core))
    for d in ((0, 1, 0), (1, 0, 0), (3, 0, 0), (2, 0, 0), (0, 0, 1)):
        greet(near_by(*d))
    kept = sum(jnp.where(needed_here(i), 1, 0) for i in range(4))
    for stage in stages:
        stage.wait()
    pl.semaphore_wait(barrier, 3 + c + 16 - kept + 5)

    sent = []

    def send(copy, when=None):
        if when is None:
            copy.start()
        else:

            @pl.when(when)
            def _():
                copy.start()

        sent.append((copy, when))

    def relay_copy(i):
        return remote(own, 32 + i, zs.at[i], zr.at[i], relay_to(i))

    urgent = ((8 - z - c) >> 1) & 3
    for step in (0, 1, 3, 2):
        i = (urgent + step) & 3
        send(relay_copy(i), (i > 0) | (c == 1))

    mate = (1 - yl) * 8 + x * 2 + c

    def slot(half, x_from, core):
        return half * 8 + x_from * 2 + core

    def row_copy(n, at, d):
        return remote(at, at, rs.at[n], rr.at[n], near_by(*d))

    def core_copy(n, at):
        return remote(at, at, ds.at[n], dr.at[n], near_by(0, 0, 1))

    send(row_copy(0, own, (0, 1, 0)))
    for n, dx in enumerate((1, 3, 2)):
        send(row_copy(1 + n, own, (dx, 0, 0)))
    send(core_copy(0, own))

    def forward(i):
        at = jnp.where(c == 0, own, 32) if i == 0 else 32 + i
        here = needed_here(i)
        for high in (0, 1):
            half = (yh + high) & 1
            for step in (1, 0):
                copy = remote(at, 16 + own, cs.at[4 * i + 2 * high + step], cr.at[own], needs(i, half, step))
                if step:
                    send(copy)
                else:
                    send(copy, jnp.logical_not(here & (half == 0)))

        @pl.when(here)
        def _():
            buf[16 + own] = buf[at]

    def across(half, k):
        for n, dx in enumerate((1, 3, 2)):
            at = slot(half, (x + 4 - dx) & 3, c)
            row_copy(1 + n + 3 * k, at, (dx, 0, 0)).wait_recv()
            send(core_copy(2 + 2 * n + k, at))

    for n, i in enumerate(NEAR):
        if i == 0:

            @pl.when(c == 1)
            def _():
                relay_copy(0).wait_recv()

        else:
            relay_copy(i).wait_recv()
        forward(i)
        if n == 0:
            row_copy(0, mate, (0, 1, 0)).wait_recv()
            for k, dx in enumerate((1, 3, 2)):
                send(row_copy(4 + k, mate, (dx, 0, 0)))
            send(core_copy(1, mate))
        if n == 1:
            across(yl, 0)
    across(1 - yl, 1)
    core_copy(0, slot(yl, x, 1 - c)).wait_recv()
    core_copy(1, slot(1 - yl, x, 1 - c)).wait_recv()
    for n, dx in enumerate((1, 3, 2)):
        for k, half in enumerate((yl, 1 - yl)):
            core_copy(2 + 2 * n + k, slot(half, (x + 4 - dx) & 3, 1 - c)).wait_recv()

    during()

    for half, step, core in pieces:
        x_from = (x + step) & 3
        at = slot(half, x_from, core)
        copy = remote(own, 16 + at, cs.at[0], cr.at[at], relay_device(half, x_from, core))
        if step == 0:

            @pl.when(jnp.logical_not(relay_is_here(half, x_from, core)))
            def _():
                copy.wait_recv()

        else:
            copy.wait_recv()
    for copy, when in sent:
        if when is None:
            copy.wait_send()
        else:

            @pl.when(when)
            def _():
                copy.wait_send()


def unpack(ref, first, flat, folded):
    for j in range(8):
        lanes = pl.ds(j * WIDTH, WIDTH)
        flat[0:128, lanes] = ref[first + j, 0:128]
        flat[128:240, lanes] = ref[first + 8 + j, 16:128]
        flat[240:248, lanes] = ref[first + j, 128:136]
        flat[248:256, lanes] = ref[first + 8 + j, 128:136]
        folded[0:16, lanes] = ref[first + 8 + j, 0:16]


def picks(shape, axis, window, last, fold):
    spot = lax.broadcasted_iota(jnp.int32, shape, axis)
    if fold:
        day = jnp.where(spot < 16, spot + 256, 1 << 20)
    else:
        day = jnp.where(
            spot < 128, spot, jnp.where(spot < 240, spot + 8, jnp.where(spot < 248, spot - 112, spot))
        )
    return jnp.where((day <= last) & (day > last - window), 1.0, 0.0).astype(F32)


def sums(flat, folded, main_mask, fold_mask, wide):
    first = jnp.zeros((16, ROWS), F32)
    second = jnp.zeros((16, ROWS), F32)
    for ref, mask in ((flat, main_mask), (folded, fold_mask)):
        block = ref[...]
        first += jnp.dot(mask, block, preferred_element_type=F32)
        wide_block = block.astype(F32)
        square = wide_block * wide_block
        high = square.astype(BF)
        low = (square - high.astype(F32)).astype(BF)
        second += jnp.dot(mask, high, preferred_element_type=F32)
        second += jnp.dot(mask, low, preferred_element_type=F32)
    scale = lax.rsqrt((second - first * first / wide) / wide + 1e-06)
    return first, scale


def gather_kernel(
    src, window, days_hbm,
    buf, left, turned, masks, folds, widths,
    days, a, a_fold, at, at_fold, small_sem, *sems,
):
    get_days = pltpu.make_async_copy(days_hbm, days, small_sem.at[0])
    get_days.start()

    def during():
        get_days.wait()
        width = window[0]
        wide = width.astype(F32)
        widths[...] = jnp.full((8, WIDTH), wide, F32)
        row = lax.broadcasted_iota(jnp.int32, (16, 256), 0)
        main = jnp.zeros((16, 256), F32)
        fold = jnp.zeros((16, 256), F32)
        for k in range(4):
            main = jnp.where(row == k, picks((16, 256), 1, width, days[k], False), main)
            fold = jnp.where(row == k, picks((16, 256), 1, width, days[k], True), fold)
            folds[2 * k] = picks((16, WIDTH), 0, width, days[k], False).astype(BF)
            folds[2 * k + 1] = picks((16, WIDTH), 0, width, days[k], True).astype(BF)
        masks[0:16, :] = main.astype(BF)
        masks[16:32, :] = fold.astype(BF)

        unpack(buf, 0, a, a_fold)
        a_fold[16:128, :] = jnp.zeros((112, ROWS), BF)
        for j in range(8):
            lanes = pl.ds(j * WIDTH, WIDTH)
            at[lanes, 0:128] = jnp.transpose(a[0:128, lanes])
            at[lanes, 128:256] = jnp.transpose(a[128:256, lanes])
            at_fold[lanes, :] = jnp.transpose(a_fold[:, lanes])
        first, scale = sums(a, a_fold.at[0:16], masks[0:16, :], masks[16:32, 0:16], wide)
        pad = jnp.zeros((96, ROWS), F32)
        turned[...] = jnp.transpose(jnp.concatenate([first, scale, pad], axis=0))
        for k in range(4):
            main = picks((1, 256), 1, width, days[k], False).astype(BF)
            fold = picks((1, 128), 1, width, days[k], True).astype(BF)
            left[k, :, 0:128] = at[:, 0:128] * main[:, 0:128] + at_fold[...] * fold
            left[k, :, 128:256] = at[:, 128:256] * main[:, 128:256]

    exchange(src, buf, *sems, during)


def gather(block, window, out_days):
    vmem = pl.BlockSpec(memory_space=pltpu.VMEM)
    hbm = pl.BlockSpec(memory_space=pltpu.HBM)
    return pl.pallas_call(
        gather_kernel,
        out_shape=(
            pltpu.VMEM((36, HALF, WIDTH), BF),
            pltpu.VMEM((4, ROWS, 256), BF),
            pltpu.VMEM((ROWS, WIDTH), F32),
            pltpu.VMEM((32, 256), BF),
            pltpu.VMEM((8, 16, WIDTH), BF),
            pltpu.VMEM((8, WIDTH), F32),
        ),
        in_specs=[hbm, pl.BlockSpec(memory_space=pltpu.SMEM), hbm],
        out_specs=(vmem,) * 6,
        scratch_shapes=[
            pltpu.SMEM((4,), jnp.int32),
            pltpu.VMEM((256, ROWS), BF),
            pltpu.VMEM((128, ROWS), BF),
            pltpu.VMEM((ROWS, 256), BF),
            pltpu.VMEM((ROWS, 128), BF),
            pltpu.SemaphoreType.DMA((1,)),
        ]
        + [pltpu.SemaphoreType.DMA((n,)) for n in (2, 4, 4, 16, 16, 7, 7, 8, 8)],
        compiler_params=pltpu.CompilerParams(collective_id=0, has_side_effects=True, vmem_limit_bytes=16 << 20),
        name="gather",
    )(block, window, out_days)


def correlate_kernel(buf, left, turned, masks, folds, widths, out, b, b_fold, bk, tiles, sem):
    wide = widths[0:1, 0:1]
    unpack(buf, 16, b, b_fold)
    first, scale = sums(b, b_fold, masks[0:16, :], masks[16:32, 0:16], wide)
    first = first / wide
    scale = scale / wide
    bk[16:256, :] = b[16:256, :]
    copies = []
    for k in range(4):
        for j in range(8):
            lanes = pl.ds(j * WIDTH, WIDTH)
            bk[0:16, lanes] = b[0:16, lanes] * folds[2 * k] + b_fold[:, lanes] * folds[2 * k + 1]
        for m in range(0, ROWS, 512):
            part = slice(m, m + 512)
            gram = jnp.dot(left[k, part, :], bk[...], preferred_element_type=F32)
            mean = turned[part, k : k + 1] * first[k : k + 1, :]
            value = (gram - mean) * turned[part, 16 + k : 17 + k] * scale[k : k + 1, :]
            tiles[k, part, :] = value.astype(BF)
            copy = pltpu.make_async_copy(
                tiles.at[k, pl.ds(m, 512)], out.at[k, pl.ds(m, 512)], sem.at[len(copies)]
            )
            copy.start()
            copies.append(copy)
    for copy in copies:
        copy.wait()


def correlate(*operands):
    return pl.pallas_call(
        correlate_kernel,
        out_shape=jax.ShapeDtypeStruct((4, ROWS, ROWS), BF),
        in_specs=[pl.BlockSpec(memory_space=pltpu.VMEM)] * 6,
        out_specs=pl.BlockSpec(memory_space=pl.ANY),
        scratch_shapes=[
            pltpu.VMEM((256, ROWS), BF),
            pltpu.VMEM((16, ROWS), BF),
            pltpu.VMEM((256, ROWS), BF),
            pltpu.VMEM((4, ROWS, ROWS), BF),
            pltpu.SemaphoreType.DMA((16,)),
        ],
        compiler_params=pltpu.CompilerParams(vmem_limit_bytes=32 << 20),
        name="correlate",
    )(*operands)


def on_device(returns, window, out_days):
    returns = pltpu.with_memory_space_constraint(returns, pltpu.HBM)
    out_days = pltpu.with_memory_space_constraint(out_days, pltpu.HBM)
    return correlate(*gather(returns, window, out_days))


def solution(mesh):
    return jax.shard_map(
        on_device,
        mesh=mesh,
        in_specs=(P("tm", ("row", "col")), P(), P()),
        out_specs=P(None, "row", ("col", "tm")),
        check_vma=False,
    )
```

```python
import jax
import jax.numpy as jnp
from jax import lax
from jax.experimental import pallas as pl
from jax.experimental.pallas import tpu as pltpu
from jax.sharding import PartitionSpec as P

MESH = pl.DeviceIdType.MESH
BF = jnp.bfloat16
F32 = jnp.float32
HALF = 136
WIDTH = 128
ROWS = 1024
NEAR = (0, 3, 1, 2)


def place():
    row = lax.axis_index("row")
    col = lax.axis_index("col")
    return col >> 1, row >> 3, lax.axis_index("tm"), row & 7, col & 1


def device(x, y_hi, y_lo, z, core):
    return {"tm": y_lo, "row": y_hi * 8 + z, "col": x * 2 + core}


def bit(value, n):
    return (value >> n) & 1


def exchange(src, buf, stage_sem, zs, zr, cs, cr, rs, rr, ds, dr, during):
    x, yh, yl, z, c = place()
    own = yl * 8 + x * 2 + c

    stages = [
        pltpu.make_async_copy(
            src.at[pl.ds(pl.multiple_of(yl * 120, 8), 16)], buf.at[own, pl.ds(0, 16)], stage_sem.at[0]
        ),
        pltpu.make_async_copy(
            src.at[pl.ds(pl.multiple_of(16 - yl * 16, 8), 120)], buf.at[own, pl.ds(16, 120)], stage_sem.at[1]
        ),
    ]
    for stage in stages:
        stage.start()

    def remote(at, to, send, recv, target):
        return pltpu.make_async_remote_copy(
            src_ref=buf.at[at],
            dst_ref=buf.at[to],
            send_sem=send,
            recv_sem=recv,
            device_id=target,
            device_id_type=MESH,
        )

    beside = 1 - 2 * c

    def relay_to(i):
        to = (z + 2 * i + c) & 7
        return device(x, (yh + bit(z, 1) + bit(to, 1)) & 1, yl, to, c)

    def relay_from(i):
        at = (z + 8 - 2 * i - c) & 7
        return at, (yh + bit(z, 1) + bit(at, 1)) & 1

    def needs(i, half, step):
        at, high = relay_from(i)
        return device(2 * high + (at >> 2), (yh + half) & 1, at & 1, (z + 8 + beside * step) & 7, bit(at, 1))

    def needed_here(i):
        at, high = relay_from(i)
        return (2 * high + (at >> 2) == x) & (at & 1 == yl) & (bit(at, 1) == c)

    wanted = 4 * (x & 1) + 2 * c + yl

    def relay_at(half, x_from, core):
        same = (z + wanted + core) & 1 == 0
        at = jnp.where(same, z, (z + 7 + 2 * core) & 7)
        return at, ((x >> 1) + bit(wanted, 1) + bit(at, 1)) & 1

    def relay_is_here(half, x_from, core):
        at, high = relay_at(half, x_from, core)
        return (at == z) & (high == yh) & (half == yl) & (x_from == x) & (core == c)

    pieces = [(half, step, core) for step in (0, 1, 3, 2) for half in (0, 1) for core in (0, 1)]

    def relay_device(half, x_from, core):
        at, high = relay_at(half, x_from, core)
        return device(x_from, high, half, at, core)

    def near_by(dx, dl, dc):
        return device((x + dx) & 3, yh, (yl + dl) & 1, z, (c + dc) & 1)

    barrier = pltpu.get_barrier_semaphore()

    def greet(target):
        pl.semaphore_signal(barrier, inc=1, device_id=target, device_id_type=MESH)

    for i in (2, 1, 3):
        at, high = relay_from(i)
        greet(device(x, high, yl, at, c))

    @pl.when(c == 1)
    def _():
        at, high = relay_from(0)
        greet(device(x, high, yl, at, c))

    for half, step, core in pieces:
        x_from = (x + step) & 3
        if step == 0:

            @pl.when(jnp.logical_not(relay_is_here(half, x_from, core)))
            def _():
                greet(relay_device(half, x_from, core))

        else:
            greet(relay_device(half, x_from, core))
    for d in ((0, 1, 0), (1, 0, 0), (3, 0, 0), (2, 0, 0), (0, 0, 1)):
        greet(near_by(*d))
    kept = sum(jnp.where(needed_here(i), 1, 0) for i in range(4))
    for stage in stages:
        stage.wait()
    pl.semaphore_wait(barrier, 3 + c + 16 - kept + 5)

    sent = []

    def send(copy, when=None):
        if when is None:
            copy.start()
        else:

            @pl.when(when)
            def _():
                copy.start()

        sent.append((copy, when))

    def relay_copy(i):
        return remote(own, 32 + i, zs.at[i], zr.at[i], relay_to(i))

    urgent = ((8 - z - c) >> 1) & 3
    for step in (0, 1, 3, 2):
        i = (urgent + step) & 3
        send(relay_copy(i), (i > 0) | (c == 1))

    mate = (1 - yl) * 8 + x * 2 + c

    def slot(half, x_from, core):
        return half * 8 + x_from * 2 + core

    def row_copy(n, at, d):
        return remote(at, at, rs.at[n], rr.at[n], near_by(*d))

    def core_copy(n, at):
        return remote(at, at, ds.at[n], dr.at[n], near_by(0, 0, 1))

    send(row_copy(0, own, (0, 1, 0)))
    for n, dx in enumerate((1, 3, 2)):
        send(row_copy(1 + n, own, (dx, 0, 0)))
    send(core_copy(0, own))

    def forward(i):
        at = jnp.where(c == 0, own, 32) if i == 0 else 32 + i
        here = needed_here(i)
        for high in (0, 1):
            half = (yh + high) & 1
            for step in (1, 0):
                copy = remote(at, 16 + own, cs.at[4 * i + 2 * high + step], cr.at[own], needs(i, half, step))
                if step:
                    send(copy)
                else:
                    send(copy, jnp.logical_not(here & (half == 0)))

        @pl.when(here)
        def _():
            buf[16 + own] = buf[at]

    def across(half, k):
        for n, dx in enumerate((1, 3, 2)):
            at = slot(half, (x + 4 - dx) & 3, c)
            row_copy(1 + n + 3 * k, at, (dx, 0, 0)).wait_recv()
            send(core_copy(2 + 2 * n + k, at))

    for n, i in enumerate(NEAR):
        if i == 0:

            @pl.when(c == 1)
            def _():
                relay_copy(0).wait_recv()

        else:
            relay_copy(i).wait_recv()
        forward(i)
        if n == 0:
            row_copy(0, mate, (0, 1, 0)).wait_recv()
            for k, dx in enumerate((1, 3, 2)):
                send(row_copy(4 + k, mate, (dx, 0, 0)))
            send(core_copy(1, mate))
        if n == 1:
            across(yl, 0)
    across(1 - yl, 1)
    core_copy(0, slot(yl, x, 1 - c)).wait_recv()
    core_copy(1, slot(1 - yl, x, 1 - c)).wait_recv()
    for n, dx in enumerate((1, 3, 2)):
        for k, half in enumerate((yl, 1 - yl)):
            core_copy(2 + 2 * n + k, slot(half, (x + 4 - dx) & 3, 1 - c)).wait_recv()

    during()

    for half, step, core in pieces:
        x_from = (x + step) & 3
        at = slot(half, x_from, core)
        copy = remote(own, 16 + at, cs.at[0], cr.at[at], relay_device(half, x_from, core))
        if step == 0:

            @pl.when(jnp.logical_not(relay_is_here(half, x_from, core)))
            def _():
                copy.wait_recv()

        else:
            copy.wait_recv()
    for copy, when in sent:
        if when is None:
            copy.wait_send()
        else:

            @pl.when(when)
            def _():
                copy.wait_send()


def unpack(ref, first, flat, folded):
    for j in range(8):
        lanes = pl.ds(j * WIDTH, WIDTH)
        flat[0:128, lanes] = ref[first + j, 0:128]
        flat[128:240, lanes] = ref[first + 8 + j, 16:128]
        flat[240:248, lanes] = ref[first + j, 128:136]
        flat[248:256, lanes] = ref[first + 8 + j, 128:136]
        folded[0:16, lanes] = ref[first + 8 + j, 0:16]


def picks(shape, axis, window, last, fold):
    spot = lax.broadcasted_iota(jnp.int32, shape, axis)
    if fold:
        day = jnp.where(spot < 16, spot + 256, 1 << 20)
    else:
        day = jnp.where(
            spot < 128, spot, jnp.where(spot < 240, spot + 8, jnp.where(spot < 248, spot - 112, spot))
        )
    return jnp.where((day <= last) & (day > last - window), 1.0, 0.0).astype(F32)


def sums(flat, folded, main_mask, fold_mask, wide):
    inner = flat[80:256, :].astype(F32)
    first = jnp.sum(inner, axis=0, keepdims=True)
    second = jnp.sum(inner * inner, axis=0, keepdims=True)
    for block, mask in ((flat[0:80, :], main_mask), (folded[...], fold_mask)):
        first += jnp.dot(mask, block, preferred_element_type=F32)[0:8]
        wide_block = block.astype(F32)
        square = wide_block * wide_block
        high = square.astype(BF)
        low = (square - high.astype(F32)).astype(BF)
        second += jnp.dot(mask, high, preferred_element_type=F32)[0:8]
        second += jnp.dot(mask, low, preferred_element_type=F32)[0:8]
    scale = lax.rsqrt((second - first * first / wide) / wide + 1e-06)
    return first, scale


def gather_kernel(
    src, window, days_hbm,
    buf, left, turned, masks, folds, widths,
    days, a, a_fold, at, at_fold, small_sem, *sems,
):
    get_days = pltpu.make_async_copy(days_hbm, days, small_sem.at[0])
    get_days.start()

    def during():
        get_days.wait()
        width = window[0]
        wide = width.astype(F32)
        widths[...] = jnp.full((8, WIDTH), wide, F32)
        row = lax.broadcasted_iota(jnp.int32, (16, 256), 0)
        main = jnp.zeros((16, 256), F32)
        fold = jnp.zeros((16, 256), F32)
        for k in range(4):
            main = jnp.where(row == k, picks((16, 256), 1, width, days[k], False), main)
            fold = jnp.where(row == k, picks((16, 256), 1, width, days[k], True), fold)
            folds[2 * k] = picks((16, WIDTH), 0, width, days[k], False).astype(BF)
            folds[2 * k + 1] = picks((16, WIDTH), 0, width, days[k], True).astype(BF)
        masks[0:16, :] = main.astype(BF)
        masks[16:32, :] = fold.astype(BF)

        unpack(buf, 0, a, a_fold)
        a_fold[16:128, :] = jnp.zeros((112, ROWS), BF)
        for j in range(8):
            lanes = pl.ds(j * WIDTH, WIDTH)
            at[lanes, 0:128] = jnp.transpose(a[0:128, lanes])
            at[lanes, 128:256] = jnp.transpose(a[128:256, lanes])
            at_fold[lanes, :] = jnp.transpose(a_fold[:, lanes])
        first, scale = sums(a, a_fold.at[0:16], masks[0:16, 0:80], masks[16:32, 0:16], wide)
        pad = jnp.zeros((112, ROWS), F32)
        turned[...] = jnp.transpose(jnp.concatenate([first, scale, pad], axis=0))
        for k in range(4):
            main = picks((1, 256), 1, width, days[k], False).astype(BF)
            fold = picks((1, 128), 1, width, days[k], True).astype(BF)
            left[k, :, 0:128] = at[:, 0:128] * main[:, 0:128] + at_fold[...] * fold
            left[k, :, 128:256] = at[:, 128:256] * main[:, 128:256]

    exchange(src, buf, *sems, during)


def gather(block, window, out_days):
    vmem = pl.BlockSpec(memory_space=pltpu.VMEM)
    hbm = pl.BlockSpec(memory_space=pltpu.HBM)
    return pl.pallas_call(
        gather_kernel,
        out_shape=(
            pltpu.VMEM((36, HALF, WIDTH), BF),
            pltpu.VMEM((4, ROWS, 256), BF),
            pltpu.VMEM((ROWS, WIDTH), F32),
            pltpu.VMEM((32, 256), BF),
            pltpu.VMEM((8, 16, WIDTH), BF),
            pltpu.VMEM((8, WIDTH), F32),
        ),
        in_specs=[hbm, pl.BlockSpec(memory_space=pltpu.SMEM), hbm],
        out_specs=(vmem,) * 6,
        scratch_shapes=[
            pltpu.SMEM((4,), jnp.int32),
            pltpu.VMEM((256, ROWS), BF),
            pltpu.VMEM((128, ROWS), BF),
            pltpu.VMEM((ROWS, 256), BF),
            pltpu.VMEM((ROWS, 128), BF),
            pltpu.SemaphoreType.DMA((1,)),
        ]
        + [pltpu.SemaphoreType.DMA((n,)) for n in (2, 4, 4, 16, 16, 7, 7, 8, 8)],
        compiler_params=pltpu.CompilerParams(collective_id=0, has_side_effects=True, vmem_limit_bytes=16 << 20),
        name="gather",
    )(block, window, out_days)


def correlate_kernel(buf, left, turned, masks, folds, widths, out, b, b_fold, bk, tiles, sem):
    wide = widths[0:1, 0:1]
    unpack(buf, 16, b, b_fold)
    first, scale = sums(b, b_fold, masks[0:16, 0:80], masks[16:32, 0:16], wide)
    first = first / wide
    scale = scale / wide
    bk[16:256, :] = b[16:256, :]
    copies = []
    for k in range(4):
        for j in range(8):
            lanes = pl.ds(j * WIDTH, WIDTH)
            bk[0:16, lanes] = b[0:16, lanes] * folds[2 * k] + b_fold[:, lanes] * folds[2 * k + 1]
        for m, height in ((0, 512), (512, 512)) if k < 3 else ((0, 512), (512, 256), (768, 256)):
            part = slice(m, m + height)
            gram = jnp.dot(left[k, part, :], bk[...], preferred_element_type=F32)
            mean = turned[part, k : k + 1] * first[k : k + 1, :]
            value = (gram - mean) * turned[part, 8 + k : 9 + k] * scale[k : k + 1, :]
            tiles[k, part, :] = value.astype(BF)
            copy = pltpu.make_async_copy(
                tiles.at[k, pl.ds(m, height)], out.at[k, pl.ds(m, height)], sem.at[len(copies)]
            )
            copy.start()
            copies.append(copy)
    for copy in copies:
        copy.wait()


def correlate(*operands):
    return pl.pallas_call(
        correlate_kernel,
        out_shape=jax.ShapeDtypeStruct((4, ROWS, ROWS), BF),
        in_specs=[pl.BlockSpec(memory_space=pltpu.VMEM)] * 6,
        out_specs=pl.BlockSpec(memory_space=pl.ANY),
        scratch_shapes=[
            pltpu.VMEM((256, ROWS), BF),
            pltpu.VMEM((16, ROWS), BF),
            pltpu.VMEM((256, ROWS), BF),
            pltpu.VMEM((4, ROWS, ROWS), BF),
            pltpu.SemaphoreType.DMA((16,)),
        ],
        compiler_params=pltpu.CompilerParams(vmem_limit_bytes=32 << 20),
        name="correlate",
    )(*operands)


def on_device(returns, window, out_days):
    returns = pltpu.with_memory_space_constraint(returns, pltpu.HBM)
    out_days = pltpu.with_memory_space_constraint(out_days, pltpu.HBM)
    return correlate(*gather(returns, window, out_days))


def solution(mesh):
    return jax.shard_map(
        on_device,
        mesh=mesh,
        in_specs=(P("tm", ("row", "col")), P(), P()),
        out_specs=P(None, "row", ("col", "tm")),
        check_vma=False,
    )
```

```python
import jax
import jax.numpy as jnp
from jax import lax
from jax.experimental import pallas as pl
from jax.experimental.pallas import tpu as pltpu
from jax.sharding import PartitionSpec as P

MESH = pl.DeviceIdType.MESH
BF = jnp.bfloat16
F32 = jnp.float32
HALF = 136
WIDTH = 128
ROWS = 1024
NEAR = (0, 3, 1, 2)


def place():
    row = lax.axis_index("row")
    col = lax.axis_index("col")
    return col >> 1, row >> 3, lax.axis_index("tm"), row & 7, col & 1


def device(x, y_hi, y_lo, z, core):
    return {"tm": y_lo, "row": y_hi * 8 + z, "col": x * 2 + core}


def bit(value, n):
    return (value >> n) & 1


def exchange(src, buf, stage_sem, zs, zr, cs, cr, rs, rr, ds, dr, during):
    x, yh, yl, z, c = place()
    own = yl * 8 + x * 2 + c

    stages = [
        pltpu.make_async_copy(
            src.at[pl.ds(pl.multiple_of(yl * 120, 8), 16)], buf.at[own, pl.ds(0, 16)], stage_sem.at[0]
        ),
        pltpu.make_async_copy(
            src.at[pl.ds(pl.multiple_of(16 - yl * 16, 8), 120)], buf.at[own, pl.ds(16, 120)], stage_sem.at[1]
        ),
    ]
    for stage in stages:
        stage.start()

    def remote(at, to, send, recv, target):
        return pltpu.make_async_remote_copy(
            src_ref=buf.at[at],
            dst_ref=buf.at[to],
            send_sem=send,
            recv_sem=recv,
            device_id=target,
            device_id_type=MESH,
        )

    beside = 1 - 2 * c

    def relay_to(i):
        to = (z + 2 * i + c) & 7
        return device(x, (yh + bit(z, 1) + bit(to, 1)) & 1, yl, to, c)

    def relay_from(i):
        at = (z + 8 - 2 * i - c) & 7
        return at, (yh + bit(z, 1) + bit(at, 1)) & 1

    def needs(i, half, step):
        at, high = relay_from(i)
        return device(2 * high + (at >> 2), (yh + half) & 1, at & 1, (z + 8 + beside * step) & 7, bit(at, 1))

    def needed_here(i):
        at, high = relay_from(i)
        return (2 * high + (at >> 2) == x) & (at & 1 == yl) & (bit(at, 1) == c)

    wanted = 4 * (x & 1) + 2 * c + yl

    def relay_at(half, x_from, core):
        same = (z + wanted + core) & 1 == 0
        at = jnp.where(same, z, (z + 7 + 2 * core) & 7)
        return at, ((x >> 1) + bit(wanted, 1) + bit(at, 1)) & 1

    def relay_is_here(half, x_from, core):
        at, high = relay_at(half, x_from, core)
        return (at == z) & (high == yh) & (half == yl) & (x_from == x) & (core == c)

    pieces = [(half, step, core) for step in (0, 1, 3, 2) for half in (0, 1) for core in (0, 1)]

    def relay_device(half, x_from, core):
        at, high = relay_at(half, x_from, core)
        return device(x_from, high, half, at, core)

    def near_by(dx, dl, dc):
        return device((x + dx) & 3, yh, (yl + dl) & 1, z, (c + dc) & 1)

    barrier = pltpu.get_barrier_semaphore()

    def greet(target):
        pl.semaphore_signal(barrier, inc=1, device_id=target, device_id_type=MESH)

    for i in (2, 1, 3):
        at, high = relay_from(i)
        greet(device(x, high, yl, at, c))

    @pl.when(c == 1)
    def _():
        at, high = relay_from(0)
        greet(device(x, high, yl, at, c))

    for half, step, core in pieces:
        x_from = (x + step) & 3
        if step == 0:

            @pl.when(jnp.logical_not(relay_is_here(half, x_from, core)))
            def _():
                greet(relay_device(half, x_from, core))

        else:
            greet(relay_device(half, x_from, core))
    for d in ((0, 1, 0), (1, 0, 0), (3, 0, 0), (2, 0, 0), (0, 0, 1)):
        greet(near_by(*d))
    kept = sum(jnp.where(needed_here(i), 1, 0) for i in range(4))
    for stage in stages:
        stage.wait()
    pl.semaphore_wait(barrier, 3 + c + 16 - kept + 5)

    sent = []

    def send(copy, when=None):
        if when is None:
            copy.start()
        else:

            @pl.when(when)
            def _():
                copy.start()

        sent.append((copy, when))

    def relay_copy(i):
        return remote(own, 32 + i, zs.at[i], zr.at[i], relay_to(i))

    for i in NEAR:
        send(relay_copy(i), c == 1 if i == 0 else None)

    mate = (1 - yl) * 8 + x * 2 + c

    def slot(half, x_from, core):
        return half * 8 + x_from * 2 + core

    def row_copy(n, at, d):
        return remote(at, at, rs.at[n], rr.at[n], near_by(*d))

    def core_copy(n, at):
        return remote(at, at, ds.at[n], dr.at[n], near_by(0, 0, 1))

    send(row_copy(0, own, (0, 1, 0)))
    for n, dx in enumerate((1, 3, 2)):
        send(row_copy(1 + n, own, (dx, 0, 0)))
    send(core_copy(0, own))

    def forward(i):
        at = jnp.where(c == 0, own, 32) if i == 0 else 32 + i
        here = needed_here(i)
        for step in (1, 0):
            for half in (1, 0):
                copy = remote(at, 16 + own, cs.at[4 * i + 2 * half + step], cr.at[own], needs(i, half, step))
                if step or half:
                    send(copy)
                else:
                    send(copy, jnp.logical_not(here))

                    @pl.when(here)
                    def _():
                        buf[16 + own] = buf[at]

    for n, i in enumerate(NEAR):
        if i == 0:

            @pl.when(c == 1)
            def _():
                relay_copy(0).wait_recv()

        else:
            relay_copy(i).wait_recv()
        forward(i)
        if n == 0:
            row_copy(0, mate, (0, 1, 0)).wait_recv()
            for k, dx in enumerate((1, 3, 2)):
                send(row_copy(4 + k, mate, (dx, 0, 0)))
            send(core_copy(1, mate))
    for n, dx in enumerate((1, 3, 2)):
        x_from = (x + 4 - dx) & 3
        for k, half in enumerate((yl, 1 - yl)):
            at = slot(half, x_from, c)
            row_copy(1 + n + 3 * k, at, (dx, 0, 0)).wait_recv()
            send(core_copy(2 + 2 * n + k, at))
    core_copy(0, slot(yl, x, 1 - c)).wait_recv()
    core_copy(1, slot(1 - yl, x, 1 - c)).wait_recv()
    for n, dx in enumerate((1, 3, 2)):
        for k, half in enumerate((yl, 1 - yl)):
            core_copy(2 + 2 * n + k, slot(half, (x + 4 - dx) & 3, 1 - c)).wait_recv()

    during()

    for half, step, core in pieces:
        x_from = (x + step) & 3
        at = slot(half, x_from, core)
        copy = remote(own, 16 + at, cs.at[0], cr.at[at], relay_device(half, x_from, core))
        if step == 0:

            @pl.when(jnp.logical_not(relay_is_here(half, x_from, core)))
            def _():
                copy.wait_recv()

        else:
            copy.wait_recv()
    for copy, when in sent:
        if when is None:
            copy.wait_send()
        else:

            @pl.when(when)
            def _():
                copy.wait_send()


def unpack(ref, first, flat, folded):
    for j in range(8):
        lanes = pl.ds(j * WIDTH, WIDTH)
        flat[0:128, lanes] = ref[first + j, 0:128]
        flat[128:240, lanes] = ref[first + 8 + j, 16:128]
        flat[240:248, lanes] = ref[first + j, 128:136]
        flat[248:256, lanes] = ref[first + 8 + j, 128:136]
        folded[0:16, lanes] = ref[first + 8 + j, 0:16]


def picks(shape, axis, window, last, fold):
    spot = lax.broadcasted_iota(jnp.int32, shape, axis)
    if fold:
        day = jnp.where(spot < 16, spot + 256, 1 << 20)
    else:
        day = jnp.where(
            spot < 128, spot, jnp.where(spot < 240, spot + 8, jnp.where(spot < 248, spot - 112, spot))
        )
    return jnp.where((day <= last) & (day > last - window), 1.0, 0.0).astype(F32)


def sums(flat, folded, main_mask, fold_mask, wide):
    inner = flat[80:256, :].astype(F32)
    first = jnp.sum(inner, axis=0, keepdims=True)
    second = jnp.sum(inner * inner, axis=0, keepdims=True)
    for block, mask in ((flat[0:80, :], main_mask), (folded[...], fold_mask)):
        first += jnp.dot(mask, block, preferred_element_type=F32)[0:8]
        wide_block = block.astype(F32)
        square = wide_block * wide_block
        high = square.astype(BF)
        low = (square - high.astype(F32)).astype(BF)
        second += jnp.dot(mask, high, preferred_element_type=F32)[0:8]
        second += jnp.dot(mask, low, preferred_element_type=F32)[0:8]
    scale = lax.rsqrt((second - first * first / wide) / wide + 1e-06)
    return first, scale


def gather_kernel(
    src, window, days_hbm,
    buf, left, turned, masks, folds, widths,
    days, a, a_fold, at, at_fold, small_sem, *sems,
):
    get_days = pltpu.make_async_copy(days_hbm, days, small_sem.at[0])
    get_days.start()

    def during():
        get_days.wait()
        width = window[0]
        wide = width.astype(F32)
        widths[...] = jnp.full((8, WIDTH), wide, F32)
        row = lax.broadcasted_iota(jnp.int32, (16, 256), 0)
        main = jnp.zeros((16, 256), F32)
        fold = jnp.zeros((16, 256), F32)
        for k in range(4):
            main = jnp.where(row == k, picks((16, 256), 1, width, days[k], False), main)
            fold = jnp.where(row == k, picks((16, 256), 1, width, days[k], True), fold)
            folds[2 * k] = picks((16, WIDTH), 0, width, days[k], False).astype(BF)
            folds[2 * k + 1] = picks((16, WIDTH), 0, width, days[k], True).astype(BF)
        masks[0:16, :] = main.astype(BF)
        masks[16:32, :] = fold.astype(BF)

        unpack(buf, 0, a, a_fold)
        a_fold[16:128, :] = jnp.zeros((112, ROWS), BF)
        for j in range(8):
            lanes = pl.ds(j * WIDTH, WIDTH)
            at[lanes, 0:128] = jnp.transpose(a[0:128, lanes])
            at[lanes, 128:256] = jnp.transpose(a[128:256, lanes])
            at_fold[lanes, :] = jnp.transpose(a_fold[:, lanes])
        first, scale = sums(a, a_fold.at[0:16], masks[0:16, 0:80], masks[16:32, 0:16], wide)
        pad = jnp.zeros((112, ROWS), F32)
        turned[...] = jnp.transpose(jnp.concatenate([first, scale, pad], axis=0))
        for k in range(4):
            main = picks((1, 256), 1, width, days[k], False).astype(BF)
            fold = picks((1, 128), 1, width, days[k], True).astype(BF)
            left[k, :, 0:128] = at[:, 0:128] * main[:, 0:128] + at_fold[...] * fold
            left[k, :, 128:256] = at[:, 128:256] * main[:, 128:256]

    exchange(src, buf, *sems, during)


def gather(block, window, out_days):
    vmem = pl.BlockSpec(memory_space=pltpu.VMEM)
    hbm = pl.BlockSpec(memory_space=pltpu.HBM)
    return pl.pallas_call(
        gather_kernel,
        out_shape=(
            pltpu.VMEM((36, HALF, WIDTH), BF),
            pltpu.VMEM((4, ROWS, 256), BF),
            pltpu.VMEM((ROWS, WIDTH), F32),
            pltpu.VMEM((32, 256), BF),
            pltpu.VMEM((8, 16, WIDTH), BF),
            pltpu.VMEM((8, WIDTH), F32),
        ),
        in_specs=[hbm, pl.BlockSpec(memory_space=pltpu.SMEM), hbm],
        out_specs=(vmem,) * 6,
        scratch_shapes=[
            pltpu.SMEM((4,), jnp.int32),
            pltpu.VMEM((256, ROWS), BF),
            pltpu.VMEM((128, ROWS), BF),
            pltpu.VMEM((ROWS, 256), BF),
            pltpu.VMEM((ROWS, 128), BF),
            pltpu.SemaphoreType.DMA((1,)),
        ]
        + [pltpu.SemaphoreType.DMA((n,)) for n in (2, 4, 4, 16, 16, 7, 7, 8, 8)],
        compiler_params=pltpu.CompilerParams(collective_id=0, has_side_effects=True, vmem_limit_bytes=16 << 20),
        name="gather",
    )(block, window, out_days)


def correlate_kernel(buf, left, turned, masks, folds, widths, out, b, b_fold, bk, tiles, sem):
    wide = widths[0:1, 0:1]
    unpack(buf, 16, b, b_fold)
    first, scale = sums(b, b_fold, masks[0:16, 0:80], masks[16:32, 0:16], wide)
    first = first / wide
    scale = scale / wide
    bk[16:256, :] = b[16:256, :]
    copies = []
    for k in range(4):
        for j in range(8):
            lanes = pl.ds(j * WIDTH, WIDTH)
            bk[0:16, lanes] = b[0:16, lanes] * folds[2 * k] + b_fold[:, lanes] * folds[2 * k + 1]
        for m, height in ((0, 512), (512, 512)) if k < 3 else ((0, 512), (512, 256), (768, 256)):
            part = slice(m, m + height)
            gram = jnp.dot(left[k, part, :], bk[...], preferred_element_type=F32)
            mean = turned[part, k : k + 1] * first[k : k + 1, :]
            value = (gram - mean) * turned[part, 8 + k : 9 + k] * scale[k : k + 1, :]
            tiles[k, part, :] = value.astype(BF)
            copy = pltpu.make_async_copy(
                tiles.at[k, pl.ds(m, height)], out.at[k, pl.ds(m, height)], sem.at[len(copies)]
            )
            copy.start()
            copies.append(copy)
    for copy in copies:
        copy.wait()


def correlate(*operands):
    return pl.pallas_call(
        correlate_kernel,
        out_shape=jax.ShapeDtypeStruct((4, ROWS, ROWS), BF),
        in_specs=[pl.BlockSpec(memory_space=pltpu.VMEM)] * 6,
        out_specs=pl.BlockSpec(memory_space=pl.ANY),
        scratch_shapes=[
            pltpu.VMEM((256, ROWS), BF),
            pltpu.VMEM((16, ROWS), BF),
            pltpu.VMEM((256, ROWS), BF),
            pltpu.VMEM((4, ROWS, ROWS), BF),
            pltpu.SemaphoreType.DMA((16,)),
        ],
        compiler_params=pltpu.CompilerParams(vmem_limit_bytes=32 << 20),
        name="correlate",
    )(*operands)


def on_device(returns, window, out_days):
    returns = pltpu.with_memory_space_constraint(returns, pltpu.HBM)
    out_days = pltpu.with_memory_space_constraint(out_days, pltpu.HBM)
    return correlate(*gather(returns, window, out_days))


def solution(mesh):
    return jax.shard_map(
        on_device,
        mesh=mesh,
        in_specs=(P("tm", ("row", "col")), P(), P()),
        out_specs=P(None, "row", ("col", "tm")),
        check_vma=False,
    )
```

```python
import jax
import jax.numpy as jnp
from jax import lax
from jax.experimental import pallas as pl
from jax.experimental.pallas import tpu as pltpu
from jax.sharding import PartitionSpec as P

MESH = pl.DeviceIdType.MESH
BF = jnp.bfloat16
F32 = jnp.float32
HALF = 136
WIDTH = 128
ROWS = 1024
NEAR = (0, 3, 1, 2)


def place():
    row = lax.axis_index("row")
    col = lax.axis_index("col")
    return col >> 1, row >> 3, lax.axis_index("tm"), row & 7, col & 1


def device(x, y_hi, y_lo, z, core):
    return {"tm": y_lo, "row": y_hi * 8 + z, "col": x * 2 + core}


def bit(value, n):
    return (value >> n) & 1


def exchange(src, buf, stage_sem, zs, zr, cs, cr, rs, rr, ds, dr, during):
    x, yh, yl, z, c = place()
    own = yl * 8 + x * 2 + c

    stages = [
        pltpu.make_async_copy(
            src.at[pl.ds(pl.multiple_of(yl * 120, 8), 16)], buf.at[own, pl.ds(0, 16)], stage_sem.at[0]
        ),
        pltpu.make_async_copy(
            src.at[pl.ds(pl.multiple_of(16 - yl * 16, 8), 120)], buf.at[own, pl.ds(16, 120)], stage_sem.at[1]
        ),
    ]
    for stage in stages:
        stage.start()

    def remote(at, to, send, recv, target):
        return pltpu.make_async_remote_copy(
            src_ref=buf.at[at],
            dst_ref=buf.at[to],
            send_sem=send,
            recv_sem=recv,
            device_id=target,
            device_id_type=MESH,
        )

    beside = 1 - 2 * c

    def relay_to(i):
        to = (z + 2 * i + c) & 7
        return device(x, (yh + bit(z, 1) + bit(to, 1)) & 1, yl, to, c)

    def relay_from(i):
        at = (z + 8 - 2 * i - c) & 7
        return at, (yh + bit(z, 1) + bit(at, 1)) & 1

    def needs(i, half, step):
        at, high = relay_from(i)
        return device(2 * high + (at >> 2), (yh + half) & 1, at & 1, (z + 8 + beside * step) & 7, bit(at, 1))

    def needed_here(i):
        at, high = relay_from(i)
        return (2 * high + (at >> 2) == x) & (at & 1 == yl) & (bit(at, 1) == c)

    wanted = 4 * (x & 1) + 2 * c + yl

    def relay_at(half, x_from, core):
        same = (z + wanted + core) & 1 == 0
        at = jnp.where(same, z, (z + 7 + 2 * core) & 7)
        return at, ((x >> 1) + bit(wanted, 1) + bit(at, 1)) & 1

    def relay_is_here(half, x_from, core):
        at, high = relay_at(half, x_from, core)
        return (at == z) & (high == yh) & (half == yl) & (x_from == x) & (core == c)

    pieces = [(half, step, core) for step in (0, 1, 3, 2) for half in (0, 1) for core in (0, 1)]

    def relay_device(half, x_from, core):
        at, high = relay_at(half, x_from, core)
        return device(x_from, high, half, at, core)

    def near_by(dx, dl, dc):
        return device((x + dx) & 3, yh, (yl + dl) & 1, z, (c + dc) & 1)

    barrier = pltpu.get_barrier_semaphore()

    def greet(target):
        pl.semaphore_signal(barrier, inc=1, device_id=target, device_id_type=MESH)

    for i in (2, 1, 3):
        at, high = relay_from(i)
        greet(device(x, high, yl, at, c))

    @pl.when(c == 1)
    def _():
        at, high = relay_from(0)
        greet(device(x, high, yl, at, c))

    for half, step, core in pieces:
        x_from = (x + step) & 3
        if step == 0:

            @pl.when(jnp.logical_not(relay_is_here(half, x_from, core)))
            def _():
                greet(relay_device(half, x_from, core))

        else:
            greet(relay_device(half, x_from, core))
    for d in ((0, 1, 0), (1, 0, 0), (3, 0, 0), (2, 0, 0), (0, 0, 1)):
        greet(near_by(*d))
    kept = sum(jnp.where(needed_here(i), 1, 0) for i in range(4))
    for stage in stages:
        stage.wait()
    pl.semaphore_wait(barrier, 3 + c + 16 - kept + 5)

    sent = []

    def send(copy, when=None):
        if when is None:
            copy.start()
        else:

            @pl.when(when)
            def _():
                copy.start()

        sent.append((copy, when))

    def relay_copy(i):
        return remote(own, 32 + i, zs.at[i], zr.at[i], relay_to(i))

    for i in NEAR:
        send(relay_copy(i), c == 1 if i == 0 else None)

    mate = (1 - yl) * 8 + x * 2 + c

    def slot(half, x_from, core):
        return half * 8 + x_from * 2 + core

    def row_copy(n, at, d):
        return remote(at, at, rs.at[n], rr.at[n], near_by(*d))

    def core_copy(n, at):
        return remote(at, at, ds.at[n], dr.at[n], near_by(0, 0, 1))

    send(row_copy(0, own, (0, 1, 0)))
    for n, dx in enumerate((1, 3, 2)):
        send(row_copy(1 + n, own, (dx, 0, 0)))
    send(core_copy(0, own))

    def forward(i):
        at = jnp.where(c == 0, own, 32) if i == 0 else 32 + i
        here = needed_here(i)
        for half in (1, 0):
            for step in (1, 0):
                copy = remote(at, 16 + own, cs.at[4 * i + 2 * half + step], cr.at[own], needs(i, half, step))
                if step or half:
                    send(copy)
                else:
                    send(copy, jnp.logical_not(here))

                    @pl.when(here)
                    def _():
                        buf[16 + own] = buf[at]

    for n, i in enumerate(NEAR):
        if i == 0:

            @pl.when(c == 1)
            def _():
                relay_copy(0).wait_recv()

        else:
            relay_copy(i).wait_recv()
        forward(i)
        if n == 0:
            row_copy(0, mate, (0, 1, 0)).wait_recv()
            for k, dx in enumerate((1, 3, 2)):
                send(row_copy(4 + k, mate, (dx, 0, 0)))
            send(core_copy(1, mate))
    for n, dx in enumerate((1, 3, 2)):
        x_from = (x + 4 - dx) & 3
        for k, half in enumerate((yl, 1 - yl)):
            at = slot(half, x_from, c)
            row_copy(1 + n + 3 * k, at, (dx, 0, 0)).wait_recv()
            send(core_copy(2 + 2 * n + k, at))
    core_copy(0, slot(yl, x, 1 - c)).wait_recv()
    core_copy(1, slot(1 - yl, x, 1 - c)).wait_recv()
    for n, dx in enumerate((1, 3, 2)):
        for k, half in enumerate((yl, 1 - yl)):
            core_copy(2 + 2 * n + k, slot(half, (x + 4 - dx) & 3, 1 - c)).wait_recv()

    during()

    for half, step, core in pieces:
        x_from = (x + step) & 3
        at = slot(half, x_from, core)
        copy = remote(own, 16 + at, cs.at[0], cr.at[at], relay_device(half, x_from, core))
        if step == 0:

            @pl.when(jnp.logical_not(relay_is_here(half, x_from, core)))
            def _():
                copy.wait_recv()

        else:
            copy.wait_recv()
    for copy, when in sent:
        if when is None:
            copy.wait_send()
        else:

            @pl.when(when)
            def _():
                copy.wait_send()


def unpack(ref, first, flat, folded):
    for j in range(8):
        lanes = pl.ds(j * WIDTH, WIDTH)
        flat[0:128, lanes] = ref[first + j, 0:128]
        flat[128:240, lanes] = ref[first + 8 + j, 16:128]
        flat[240:248, lanes] = ref[first + j, 128:136]
        flat[248:256, lanes] = ref[first + 8 + j, 128:136]
        folded[0:16, lanes] = ref[first + 8 + j, 0:16]


def picks(shape, axis, window, last, fold):
    spot = lax.broadcasted_iota(jnp.int32, shape, axis)
    if fold:
        day = jnp.where(spot < 16, spot + 256, 1 << 20)
    else:
        day = jnp.where(
            spot < 128, spot, jnp.where(spot < 240, spot + 8, jnp.where(spot < 248, spot - 112, spot))
        )
    return jnp.where((day <= last) & (day > last - window), 1.0, 0.0).astype(F32)


def sums(flat, folded, main_mask, fold_mask, wide):
    inner = flat[80:256, :].astype(F32)
    first = jnp.sum(inner, axis=0, keepdims=True)
    second = jnp.sum(inner * inner, axis=0, keepdims=True)
    for block, mask in ((flat[0:80, :], main_mask), (folded[...], fold_mask)):
        first += jnp.dot(mask, block, preferred_element_type=F32)[0:8]
        wide_block = block.astype(F32)
        square = wide_block * wide_block
        high = square.astype(BF)
        low = (square - high.astype(F32)).astype(BF)
        second += jnp.dot(mask, high, preferred_element_type=F32)[0:8]
        second += jnp.dot(mask, low, preferred_element_type=F32)[0:8]
    scale = lax.rsqrt((second - first * first / wide) / wide + 1e-06)
    return first, scale


def gather_kernel(
    src, window, days_hbm,
    buf, left, turned, masks, folds, widths,
    days, a, a_fold, at, at_fold, small_sem, *sems,
):
    get_days = pltpu.make_async_copy(days_hbm, days, small_sem.at[0])
    get_days.start()

    def during():
        get_days.wait()
        width = window[0]
        wide = width.astype(F32)
        widths[...] = jnp.full((8, WIDTH), wide, F32)
        row = lax.broadcasted_iota(jnp.int32, (16, 256), 0)
        main = jnp.zeros((16, 256), F32)
        fold = jnp.zeros((16, 256), F32)
        for k in range(4):
            main = jnp.where(row == k, picks((16, 256), 1, width, days[k], False), main)
            fold = jnp.where(row == k, picks((16, 256), 1, width, days[k], True), fold)
            folds[2 * k] = picks((16, WIDTH), 0, width, days[k], False).astype(BF)
            folds[2 * k + 1] = picks((16, WIDTH), 0, width, days[k], True).astype(BF)
        masks[0:16, :] = main.astype(BF)
        masks[16:32, :] = fold.astype(BF)

        unpack(buf, 0, a, a_fold)
        a_fold[16:128, :] = jnp.zeros((112, ROWS), BF)
        for j in range(8):
            lanes = pl.ds(j * WIDTH, WIDTH)
            at[lanes, 0:128] = jnp.transpose(a[0:128, lanes])
            at[lanes, 128:256] = jnp.transpose(a[128:256, lanes])
            at_fold[lanes, :] = jnp.transpose(a_fold[:, lanes])
        first, scale = sums(a, a_fold.at[0:16], masks[0:16, 0:80], masks[16:32, 0:16], wide)
        pad = jnp.zeros((112, ROWS), F32)
        turned[...] = jnp.transpose(jnp.concatenate([first, scale, pad], axis=0))
        for k in range(4):
            main = picks((1, 256), 1, width, days[k], False).astype(BF)
            fold = picks((1, 128), 1, width, days[k], True).astype(BF)
            left[k, :, 0:128] = at[:, 0:128] * main[:, 0:128] + at_fold[...] * fold
            left[k, :, 128:256] = at[:, 128:256] * main[:, 128:256]

    exchange(src, buf, *sems, during)


def gather(block, window, out_days):
    vmem = pl.BlockSpec(memory_space=pltpu.VMEM)
    hbm = pl.BlockSpec(memory_space=pltpu.HBM)
    return pl.pallas_call(
        gather_kernel,
        out_shape=(
            pltpu.VMEM((36, HALF, WIDTH), BF),
            pltpu.VMEM((4, ROWS, 256), BF),
            pltpu.VMEM((ROWS, WIDTH), F32),
            pltpu.VMEM((32, 256), BF),
            pltpu.VMEM((8, 16, WIDTH), BF),
            pltpu.VMEM((8, WIDTH), F32),
        ),
        in_specs=[hbm, pl.BlockSpec(memory_space=pltpu.SMEM), hbm],
        out_specs=(vmem,) * 6,
        scratch_shapes=[
            pltpu.SMEM((4,), jnp.int32),
            pltpu.VMEM((256, ROWS), BF),
            pltpu.VMEM((128, ROWS), BF),
            pltpu.VMEM((ROWS, 256), BF),
            pltpu.VMEM((ROWS, 128), BF),
            pltpu.SemaphoreType.DMA((1,)),
        ]
        + [pltpu.SemaphoreType.DMA((n,)) for n in (2, 4, 4, 16, 16, 7, 7, 8, 8)],
        compiler_params=pltpu.CompilerParams(collective_id=0, has_side_effects=True, vmem_limit_bytes=16 << 20),
        name="gather",
    )(block, window, out_days)


def correlate_kernel(buf, left, turned, masks, folds, widths, out, b, b_fold, bk, tiles, sem):
    wide = widths[0:1, 0:1]
    unpack(buf, 16, b, b_fold)
    first, scale = sums(b, b_fold, masks[0:16, 0:80], masks[16:32, 0:16], wide)
    first = first / wide
    scale = scale / wide
    bk[16:256, :] = b[16:256, :]
    copies = []
    for k in range(4):
        for j in range(8):
            lanes = pl.ds(j * WIDTH, WIDTH)
            bk[0:16, lanes] = b[0:16, lanes] * folds[2 * k] + b_fold[:, lanes] * folds[2 * k + 1]
        for m, height in ((0, 512), (512, 512)) if k < 3 else ((0, 512), (512, 256), (768, 256)):
            part = slice(m, m + height)
            gram = jnp.dot(left[k, part, :], bk[...], preferred_element_type=F32)
            mean = turned[part, k : k + 1] * first[k : k + 1, :]
            value = (gram - mean) * turned[part, 8 + k : 9 + k] * scale[k : k + 1, :]
            tiles[k, part, :] = value.astype(BF)
            copy = pltpu.make_async_copy(
                tiles.at[k, pl.ds(m, height)], out.at[k, pl.ds(m, height)], sem.at[len(copies)]
            )
            copy.start()
            copies.append(copy)
    for copy in copies:
        copy.wait()


def correlate(*operands):
    return pl.pallas_call(
        correlate_kernel,
        out_shape=jax.ShapeDtypeStruct((4, ROWS, ROWS), BF),
        in_specs=[pl.BlockSpec(memory_space=pltpu.VMEM)] * 6,
        out_specs=pl.BlockSpec(memory_space=pl.ANY),
        scratch_shapes=[
            pltpu.VMEM((256, ROWS), BF),
            pltpu.VMEM((16, ROWS), BF),
            pltpu.VMEM((256, ROWS), BF),
            pltpu.VMEM((4, ROWS, ROWS), BF),
            pltpu.SemaphoreType.DMA((16,)),
        ],
        compiler_params=pltpu.CompilerParams(vmem_limit_bytes=32 << 20),
        name="correlate",
    )(*operands)


def on_device(returns, window, out_days):
    returns = pltpu.with_memory_space_constraint(returns, pltpu.HBM)
    out_days = pltpu.with_memory_space_constraint(out_days, pltpu.HBM)
    return correlate(*gather(returns, window, out_days))


def solution(mesh):
    return jax.shard_map(
        on_device,
        mesh=mesh,
        in_specs=(P("tm", ("row", "col")), P(), P()),
        out_specs=P(None, "row", ("col", "tm")),
        check_vma=False,
    )
```
